32 devices in a mesh: groups: 2 (over y), dp: 4 (over x, core), tensor: 4 (over z).
Axes of the slice: x: 2, y: 2, z: 4, core: 2. Of those that a mesh axis runs over, the one named last changes fastest.
Arguments:
- query: bfloat16 [4096, 512], P(('groups', 'dp'), 'tensor'), parts along dimension 0, may hold values from -4.5 to 4.5
- keys: bfloat16 [4096, 512], P(('groups', 'dp'), 'tensor'), parts along dimension 0, may hold values from -4.5 to 4.5
- values: bfloat16 [4096, 512], P(('groups', 'dp'), 'tensor'), parts along dimension 0, may hold values from -6 to 6
- upstream: bfloat16 [4096, 8192], P(('groups', 'dp', 'tensor')), parts along dimension 0, may hold values from -6 to 6
- projection: bfloat16 [512, 8192], P('tensor', 'dp'), may hold values from -0.0625 to 0.0625
- lengths: int32 [8, 8], P(('groups', 'dp')), parts along dimension 0, may hold values from 1 to 256, 512 in all within a row
Outputs:
- grad_query: bfloat16 [4096, 512], P(('groups', 'dp'), 'tensor'), parts along dimension 0
- grad_keys: bfloat16 [4096, 512], P(('groups', 'dp'), 'tensor'), parts along dimension 0
- grad_values: bfloat16 [4096, 512], P(('groups', 'dp'), 'tensor'), parts along dimension 0
- grad_projection: float32 [1024, 8192], P(('groups', 'tensor'), 'dp'), parts along dimension 0
The draws below stay inside these ranges and needn't reach their ends.
There are 2 independent parts, one for each index of `groups`. The reference program is written for one: setup_inputs(seed, part) draws one part's arguments, and reference() takes and returns one part's arrays. A program takes and returns all parts, laid end to end along the dimension named above; an argument that names none is the same for every part. Nothing has to cross between parts.
Inputs may be any that keep to these rules, and one draw needn't show every extreme that they name: Each row holds the lengths of the 8 documents of one sequence in order; they sum to 512 and the largest is exactly 256.
All inputs are finite; a program needn't handle non-finite values.
Results may differ from the reference program's by a relative error of at most 0.014.
Values may be sent and summed in bfloat16 or wider, within the bound.
A program may use at most 64 MiB of HBM per device.

```python
import math
import jax
import jax.numpy as jnp
import numpy as np
from jax import lax

D = 8192
HD = 128
LEN = 512
SEGS = 8
HEADS = 4
SEQS = 4
TOKENS = 2048


def drawn_pair(key):
    shape = (TOKENS, HEADS * HD)
    key_query, key_keys = jax.random.split(key, 2)
    query_draw = jnp.clip(jax.random.normal(key_query, shape, jnp.float32), -4.5, 4.5)
    keys_draw = jnp.clip(jax.random.normal(key_keys, shape, jnp.float32), -4.5, 4.5)
    return (query_draw, keys_draw)


def draw_query(key, part):
    return drawn_pair(jax.random.fold_in(key, 11))[0].astype(jnp.bfloat16)


def draw_keys(key, part):
    return drawn_pair(jax.random.fold_in(key, 11))[1].astype(jnp.bfloat16)


def strengthened(values, key, source, target, parts, factor):
    owner, partner = [(jnp.arange(values.shape[position]) // (values.shape[position] // parts)).reshape([-1 if axis == position else 1 for axis in range(values.ndim)]) for position in (source, target)]
    chosen = jax.random.permutation(key, parts)[partner]
    strong = (owner == chosen) | (owner == (partner + parts // 2) % parts)
    return jnp.where(strong, factor * values, values)


def block_scale(stream_key, shape, cuts, least, top_value):
    loudness = 1.0
    for axis_at, parts in cuts:
        draws = jax.random.uniform(jax.random.fold_in(jax.random.fold_in(stream_key, 6), axis_at), (parts,), jnp.float32, least / len(cuts), top_value / len(cuts))
        loudness = loudness * jnp.repeat(jnp.exp(draws), shape[axis_at] // parts).reshape((-1,) + (1,) * (len(shape) - 1 - axis_at))
    return loudness


def split_up(number_of, total, limit, slope):
    portions = [(1 << 20) // math.isqrt(grade ** slope) + 1 for grade in range(2, number_of + 1)]
    surplus, holding = total - limit - (number_of - 1), [1] * (number_of - 1)
    while surplus > 0:
        free = [i for i in range(number_of - 1) if holding[i] < limit]
        mass, budget = sum([portions[i] for i in free]), surplus
        for i in free:
            extra = min(limit - holding[i], max(1, budget * portions[i] // mass), surplus)
            holding[i] = holding[i] + extra
            surplus = surplus - extra
    return np.array([limit] + holding)


def uneven_parts(key, amount, total, reach, skew):
    if amount == 2:
        one = jax.random.randint(key, (), max(1, total - reach), min(reach, total - 1) + 1)
        return jnp.stack([one, total - one])
    sizes = jnp.asarray(split_up(amount, total, reach, skew), jnp.int32)
    twos = (amount - 1) // 2
    source_of, sink = sizes[1:1 + 2 * twos:2], sizes[2:2 + 2 * twos:2]
    slack = jnp.minimum(source_of - 1, reach - sink)
    shifted = jax.random.randint(jax.random.fold_in(key, 1), (twos,), 0, 1 << 20) % (slack + 1)
    sizes = sizes.at[1:1 + 2 * twos:2].set(source_of - shifted).at[2:2 + 2 * twos:2].set(sink + shifted)
    return sizes[jax.random.permutation(jax.random.fold_in(key, 2), amount)]


def noise(rng, extent, scale, bound, pieces=(), kind=jnp.bfloat16):
    values = scale * jax.random.normal(rng, extent, jnp.float32)
    if pieces:
        values = values * block_scale(rng, extent, pieces, -0.22, 0.18)
    return jnp.clip(values, -bound, bound).astype(kind)


def bell_draw_with(rng, dims, scale, most, cuts, heavy, kind=jnp.bfloat16):
    result = scale * jax.random.normal(rng, dims, jnp.float32)
    if cuts:
        result = result * block_scale(rng, dims, cuts, -0.22, 0.18)
    return jnp.clip(strengthened(result, jax.random.fold_in(rng, 3), *heavy), -most, most).astype(kind)


def setup_inputs(seed: int = 0, part: int = 0) -> dict:
    arg_keys = jax.random.split(jax.random.key(seed), 7)
    own_keys = jax.random.split(jax.random.fold_in(arg_keys[6], part), 7)
    query = draw_query(jax.random.fold_in(jax.random.fold_in(arg_keys[6], part), 71), part)
    keys = draw_keys(jax.random.fold_in(jax.random.fold_in(arg_keys[6], part), 71), part)
    values = noise(own_keys[2], (TOKENS, HEADS * HD), 1.0, 6.0, ((0, 4), (1, 4)))
    upstream = bell_draw_with(own_keys[3], (TOKENS, D), 1.0, 6.0, ((0, 16),), (0, 1, 16, 2.0))
    projection = noise(arg_keys[4], (HEADS * HD, D), D ** -0.5, 0.0625, ((0, 4), (1, 4)))
    lengths = jax.vmap(lambda own: uneven_parts(own, SEGS, LEN, LEN // 2, 2))(jax.random.split(own_keys[5], SEQS)).reshape((SEQS, SEGS)).astype(jnp.int32)
    return {"query": query, "keys": keys, "values": values, "upstream": upstream, "projection": projection, "lengths": lengths}


def sequence_mask(length_row):
    segment_ends = jnp.cumsum(length_row)
    places = jnp.arange(LEN, dtype=jnp.int32)
    labels = jnp.sum((segment_ends[None, :] <= places[:, None]).astype(jnp.int32), axis=1)
    same = labels[:, None] == labels[None, :]
    return jnp.logical_and(same, places[None, :] <= places[:, None])


def reference(query, keys, values, upstream, projection, lengths):
    scaling = HD ** -0.5
    width = HEADS * HD

    def one_sequence(carry, index):
        start = (index * LEN).astype(jnp.int32)
        query_rows = lax.dynamic_slice_in_dim(query, start, LEN, 0)
        key_rows = lax.dynamic_slice_in_dim(keys, start, LEN, 0)
        value_rows = lax.dynamic_slice_in_dim(values, start, LEN, 0)
        upstream_rows = lax.dynamic_slice_in_dim(upstream, start, LEN, 0)
        length_row = lax.dynamic_index_in_dim(lengths, index, 0, keepdims=False)
        allowed = sequence_mask(length_row)
        query_heads = query_rows.reshape(LEN, HEADS, HD).astype(jnp.float32)
        key_heads = key_rows.reshape(LEN, HEADS, HD).astype(jnp.float32)
        value_heads = value_rows.reshape(LEN, HEADS, HD).astype(jnp.float32)
        scores = jnp.einsum("qhd,khd->hqk", query_heads, key_heads) * scaling
        scores = jnp.where(allowed[None], scores, -1e30)
        row_max = jnp.max(scores, axis=2, keepdims=True)
        exponent = jnp.exp(scores - row_max)
        probs = exponent / jnp.sum(exponent, axis=2, keepdims=True)
        probs_low = probs.astype(jnp.bfloat16)
        attended = jnp.einsum("hqk,khd->qhd", probs_low.astype(jnp.float32), value_heads)
        attended = attended.astype(jnp.bfloat16).reshape(LEN, width)
        out_grad = jnp.dot(upstream_rows, projection.T, preferred_element_type=jnp.float32).astype(jnp.bfloat16)
        partial_grad = jnp.dot(attended.T, upstream_rows, preferred_element_type=jnp.float32)
        grad_heads = out_grad.reshape(LEN, HEADS, HD).astype(jnp.float32)
        grad_values = jnp.einsum("hqk,qhd->khd", probs_low.astype(jnp.float32), grad_heads).astype(jnp.bfloat16)
        grad_probs = jnp.einsum("qhd,khd->hqk", grad_heads, value_heads)
        delta = jnp.sum(probs * grad_probs, axis=2, keepdims=True)
        grad_scores = (probs * (grad_probs - delta) * scaling).astype(jnp.bfloat16).astype(jnp.float32)
        grad_query = jnp.einsum("hqk,khd->qhd", grad_scores, key_heads).astype(jnp.bfloat16)
        grad_keys = jnp.einsum("hqk,qhd->khd", grad_scores, query_heads).astype(jnp.bfloat16)
        outputs = (grad_query.reshape(LEN, width), grad_keys.reshape(LEN, width), grad_values.reshape(LEN, width))
        return carry + partial_grad, outputs

    initial = jnp.zeros((width, D), jnp.float32)
    indices = jnp.arange(SEQS, dtype=jnp.int32)
    grad_projection, stacked = lax.scan(one_sequence, initial, indices)
    grad_query = stacked[0].reshape(TOKENS, width)
    grad_keys = stacked[1].reshape(TOKENS, width)
    grad_values = stacked[2].reshape(TOKENS, width)
    return grad_query, grad_keys, grad_values, grad_projection
```

```python
import functools

import jax
import jax.numpy as jnp
from jax import lax
from jax.experimental import pallas as pl
from jax.experimental.pallas import tpu as pltpu
from jax.sharding import PartitionSpec as P

HD = 128
MESH = pl.DeviceIdType.MESH
LANES = 128
CHUNKS = 4
HALVES = 2
MOST_STEPS = 8
F32 = jnp.float32
BF16 = jnp.bfloat16


def sequence_mask(length_row, row_count):
    segment_ends = jnp.cumsum(length_row)
    places = jnp.arange(row_count, dtype=jnp.int32)
    labels = jnp.sum((segment_ends[None, :] <= places[:, None]).astype(jnp.int32), axis=1)
    same = labels[:, None] == labels[None, :]
    return jnp.logical_and(same, places[None, :] <= places[:, None])


def plain_shards(query, keys, values, upstream, projection, lengths):
    row_count, width = query.shape
    head_count = width // HD
    scaling = HD ** (-0.5)
    allowed = sequence_mask(lengths[0], row_count)
    query_heads = query.reshape(row_count, head_count, HD)
    key_heads = keys.reshape(row_count, head_count, HD)
    value_heads = values.reshape(row_count, head_count, HD)
    scores = (
        jnp.einsum("qhd,khd->hqk", query_heads, key_heads, preferred_element_type=jnp.float32)
        * scaling
    )
    scores = jnp.where(allowed[None], scores, -1e30)
    row_max = jnp.max(scores, axis=2, keepdims=True)
    exponent = jnp.exp(scores - row_max)
    probs = exponent / jnp.sum(exponent, axis=2, keepdims=True)
    probs_low = probs.astype(jnp.bfloat16)
    attended = jnp.einsum(
        "hqk,khd->qhd", probs_low, value_heads, preferred_element_type=jnp.float32
    )
    attended = attended.astype(jnp.bfloat16).reshape(row_count, width)
    full_projection = lax.all_gather(projection, "dp", axis=1, tiled=True)
    gathered = lax.all_gather(upstream, "tensor", axis=0, tiled=True)
    out_total = lax.dot_general(
        gathered, full_projection, (((1,), (1,)), ((), ())), preferred_element_type=jnp.float32
    )
    partial_grad = lax.dot_general(
        attended, gathered, (((0,), (0,)), ((), ())), preferred_element_type=jnp.float32
    )
    grad_projection = lax.psum_scatter(
        partial_grad.astype(jnp.bfloat16), "dp", scatter_dimension=1, tiled=True
    ).astype(jnp.float32)
    out_grad = out_total.astype(jnp.bfloat16)
    grad_heads = out_grad.reshape(row_count, head_count, HD)
    grad_values = jnp.einsum(
        "hqk,qhd->khd", probs_low, grad_heads, preferred_element_type=jnp.float32
    ).astype(jnp.bfloat16)
    grad_probs = jnp.einsum(
        "qhd,khd->hqk", grad_heads, value_heads, preferred_element_type=jnp.float32
    )
    delta = jnp.sum(probs * grad_probs, axis=2, keepdims=True)
    grad_scores = (probs * (grad_probs - delta) * scaling).astype(jnp.bfloat16)
    grad_query = jnp.einsum(
        "hqk,khd->qhd", grad_scores, key_heads, preferred_element_type=jnp.float32
    ).astype(jnp.bfloat16)
    grad_keys = jnp.einsum(
        "hqk,qhd->khd", grad_scores, query_heads, preferred_element_type=jnp.float32
    ).astype(jnp.bfloat16)
    return (
        grad_query.reshape(row_count, width),
        grad_keys.reshape(row_count, width),
        grad_values.reshape(row_count, width),
        grad_projection,
    )


def dot(a, b, over_a, over_b):
    return lax.dot_general(
        a, b, (((over_a,), (over_b,)), ((), ())), preferred_element_type=F32
    )


def kernel(
    seqs, line, chunks,
    query, keys, values, upstream, projection, lengths,
    grad_query, grad_keys, grad_values, grad_projection,
    probs_ref, att_own, att_all, up_all, proj_all, part, part_in, og_own, og_in, stage, landed,
    up_send, up_recv, right_send, left_send, proj_recv, att_send, att_recv, spread_send,
    spread_recv, part_send, part_recv, og_send, og_recv, sum_send, sum_recv,
):
    d = lax.axis_index("dp")
    t = lax.axis_index("tensor")
    total = query.shape[0]
    rows, _ = upstream.shape
    high, features = projection.shape
    wide = features // chunks
    half = high // HALVES
    scaling = HD ** (-0.5)
    pending = []

    def copy(src, dst, send_sem, recv_sem, to_d, to_t):
        return pltpu.make_async_remote_copy(
            src_ref=src, dst_ref=dst, send_sem=send_sem, recv_sem=recv_sem,
            device_id={"dp": to_d, "tensor": to_t}, device_id_type=MESH,
        )

    barrier = pltpu.get_barrier_semaphore()
    for k in range(1, seqs):
        pl.semaphore_signal(
            barrier, inc=1, device_id={"dp": lax.rem(d + k, seqs), "tensor": t},
            device_id_type=MESH,
        )
    for k in range(1, line):
        pl.semaphore_signal(
            barrier, inc=1, device_id={"dp": d, "tensor": lax.rem(t + k, line)},
            device_id_type=MESH,
        )
    pl.semaphore_wait(barrier, seqs + line - 2)

    others = [lax.rem(d + k, seqs) for k in range(1, seqs)]
    peers = [lax.rem(t + k, line) for k in range(1, line)]
    mine = pl.ds(pl.multiple_of(d * rows, rows), rows)
    right = jnp.minimum(t + 1, line - 1)
    left = jnp.maximum(t - 1, 0)

    def send_upstream(c):
        for o in others:
            off = pl.multiple_of(o * features + c * wide, wide)
            one = copy(
                upstream.at[:, pl.ds(off, wide)], up_all.at[c, mine],
                up_send.at[o, c], up_recv.at[d, c], o, t,
            )
            one.start()
            pending.append((None, one))

    waited = set()

    def wait_upstream(c):
        if c in waited:
            return
        waited.add(c)
        for o in others:
            dst = up_all.at[c, pl.ds(pl.multiple_of(o * rows, rows), rows)]
            copy(dst, dst, up_send.at[o, c], up_recv.at[o, c], o, t).wait_recv()

    def block(j, p):
        return proj_all.at[pl.ds(pl.multiple_of(j * high + p * half, half), half)]

    def proj_send(j, p, source, where, toward):
        sems = right_send if toward is right else left_send
        one = copy(source, block(j, p), sems.at[j, p], proj_recv.at[j, p], d, toward)

        @pl.when(where)
        def _():
            one.start()

        pending.append((where, one))

    def proj_own(p):
        source = projection.at[pl.ds(p * half, half)]
        proj_send(t, p, source, t < line - 1, right)
        proj_send(t, p, source, t > 0, left)

    def proj_step(k):
        for p in range(HALVES):
            from_left, from_right = jnp.maximum(t - k, 0), jnp.minimum(t + k, line - 1)
            for j, here, toward, on in (
                (from_left, t >= k, right, t < line - 1),
                (from_right, t + k < line, left, t > 0),
            ):
                dst = block(j, p)

                @pl.when(here)
                def _(dst=dst, j=j):
                    copy(dst, dst, right_send.at[j, p], proj_recv.at[j, p], d, right).wait_recv()

                if k < line - 1:
                    proj_send(j, p, dst, jnp.logical_and(here, on), toward)

    early = max(1, chunks // 2)
    for c in range(early):
        send_upstream(c)
    proj_own(0)

    ends = []
    sofar = lengths[0, 0]
    for n in range(lengths.shape[1]):
        ends.append(sofar)
        if n + 1 < lengths.shape[1]:
            sofar = sofar + lengths[0, n + 1]
    down = lax.broadcasted_iota(jnp.int32, (total, 1), 0)
    across = lax.broadcasted_iota(jnp.int32, (1, total), 1)
    label_down = sum((down >= e).astype(jnp.int32) for e in ends)
    label_across = sum((across >= e).astype(jnp.int32) for e in ends)
    for q in range(line):
        span = slice(q * rows, (q + 1) * rows)
        scores = dot(query[span, :], keys[...], 1, 1) * scaling
        allowed = jnp.logical_and(label_down[span] == label_across, across <= down[span])
        scores = jnp.where(allowed, scores, -1e30)
        exponent = jnp.exp(scores - jnp.max(scores, axis=1, keepdims=True))
        probs = exponent / jnp.sum(exponent, axis=1, keepdims=True)
        probs_ref[span, :] = probs
        att_own[q] = dot(probs.astype(BF16), values[...], 1, 0).astype(BF16)
    att_all[t, mine] = att_own[t]
    for o in peers:
        one = copy(
            att_own.at[o], att_all.at[t, mine], att_send.at[o], att_recv.at[t], d, o
        )
        one.start()
        pending.append((None, one))
    for p in range(1, HALVES):
        proj_own(p)
    for c in range(chunks):
        up_all[c, mine] = upstream[:, pl.ds(pl.multiple_of(d * features + c * wide, wide), wide)]
    proj_all[pl.ds(pl.multiple_of(t * high, high), high), :] = projection[...]
    for o in peers:
        dst = att_all.at[o, mine]
        copy(dst, dst, att_send.at[o], att_recv.at[o], d, o).wait_recv()
    for o in others:
        one = copy(
            att_all.at[:, mine], att_all.at[:, mine], spread_send.at[o], spread_recv.at[d], o, t
        )
        one.start()
        pending.append((None, one))
    for c in range(early, chunks):
        send_upstream(c)
    proj_step(1)
    for o in others:
        dst = att_all.at[:, pl.ds(pl.multiple_of(o * rows, rows), rows)]
        copy(dst, dst, spread_send.at[o], spread_recv.at[o], o, t).wait_recv()

    def sum_chunk(c):
        wait_upstream(c)
        for k in range(line - 1, 0, -1):
            for way, head, go, first, toward in (
                (0, jnp.minimum(t + k, line - 1), t + k < line, t == 0, right),
                (1, jnp.maximum(t - k, 0), t >= k, t == line - 1, left),
            ):
                one = copy(
                    stage.at[way, head, c], landed.at[way, head, c],
                    sum_send.at[way, head, c], sum_recv.at[way, head, c], d, toward,
                )

                @pl.when(go)
                def _(way=way, head=head, first=first, one=one):
                    term = dot(att_all[head], up_all[c], 0, 0)

                    @pl.when(first)
                    def _():
                        stage[way, head, c] = term.astype(BF16)

                    @pl.when(jnp.logical_not(first))
                    def _():
                        one.wait_recv()
                        stage[way, head, c] = (
                            term + landed[way, head, c].astype(F32)
                        ).astype(BF16)

                    one.start()

                pending.append((go, one))

    def own_chunk(c):
        cols = slice(c * wide, (c + 1) * wide)
        grad_projection[:, cols] = dot(att_all[t], up_all[c], 0, 0)
        for way, there in ((0, t > 0), (1, t < line - 1)):
            dst = landed.at[way, t, c]

            @pl.when(there)
            def _(way=way, dst=dst):
                copy(
                    dst, dst, sum_send.at[way, t, c], sum_recv.at[way, t, c], d, right
                ).wait_recv()
                grad_projection[:, cols] += landed[way, t, c].astype(F32)

    def out_partials():
        for c in range(chunks):
            wait_upstream(c)
        for o in others + [d]:
            at = pl.ds(pl.multiple_of(o * rows, rows), rows)
            piece = dot(up_all[0, at], proj_all[:, :wide], 1, 1)
            for c in range(1, chunks):
                piece += dot(up_all[c, at], proj_all[:, c * wide:(c + 1) * wide], 1, 1)
            if o is d:
                part_in[d] = piece.astype(BF16)
                continue
            part[o] = piece.astype(BF16)
            one = copy(part.at[o], part_in.at[d], part_send.at[o], part_recv.at[d], o, t)
            one.start()
            pending.append((None, one))

    def out_sum():
        for o in others:
            dst = part_in.at[o]
            copy(dst, dst, part_send.at[o], part_recv.at[o], o, t).wait_recv()
        whole = sum(part_in[n].astype(F32) for n in range(seqs)).astype(BF16)
        for q in range(line):
            og_own[q] = whole[:, q * HD:(q + 1) * HD]
        og_in[t] = og_own[t]
        for o in peers:
            one = copy(og_own.at[o], og_in.at[t], og_send.at[o], og_recv.at[t], d, o)
            one.start()
            pending.append((None, one))

    for c in range(chunks):
        sum_chunk(c)
        if c == 0:
            for k in range(2, line):
                proj_step(k)
        if c == max(0, chunks - 3):
            out_partials()
        if c == max(0, chunks - 2):
            out_sum()

    for o in peers:
        dst = og_in.at[o]
        copy(dst, dst, og_send.at[o], og_recv.at[o], d, o).wait_recv()
    grads = [og_in[q] for q in range(line)]
    gv = 0.0
    gk = 0.0
    for q in range(line):
        span = slice(q * rows, (q + 1) * rows)
        probs = probs_ref[span, :]
        gv = gv + dot(probs.astype(BF16), grads[q], 0, 0)
        grad_probs = dot(grads[q], values[...], 1, 1)
        delta = jnp.sum(probs * grad_probs, axis=1, keepdims=True)
        grad_scores = (probs * (grad_probs - delta) * scaling).astype(BF16)
        grad_query[span, :] = dot(grad_scores, keys[...], 1, 0).astype(BF16)
        gk = gk + dot(grad_scores, query[span, :], 0, 0)
    grad_values[...] = gv.astype(BF16)
    grad_keys[...] = gk.astype(BF16)
    for c in range(chunks):
        own_chunk(c)

    for where, one in pending:
        if where is None:
            one.wait_send()
        else:

            @pl.when(where)
            def _(one=one):
                one.wait_send()


def fused_shards(seqs, line, query, keys, values, upstream, projection, lengths):
    total, width = query.shape
    rows = upstream.shape[0]
    high, features = projection.shape
    chunks = CHUNKS
    wide = features // chunks
    dma = pltpu.SemaphoreType.DMA
    vmem = pltpu.VMEM
    whole = pl.BlockSpec(memory_space=pltpu.VMEM)
    return pl.pallas_call(
        functools.partial(kernel, seqs, line, chunks),
        out_shape=(
            jax.ShapeDtypeStruct(query.shape, BF16),
            jax.ShapeDtypeStruct(query.shape, BF16),
            jax.ShapeDtypeStruct(query.shape, BF16),
            jax.ShapeDtypeStruct(projection.shape, F32),
        ),
        in_specs=[whole] * 5 + [pl.BlockSpec(memory_space=pltpu.SMEM)],
        out_specs=(whole,) * 4,
        scratch_shapes=[
            vmem((total, total), F32),
            vmem((line, rows, width), BF16),
            vmem((line, seqs * rows, width), BF16),
            vmem((chunks, seqs * rows, wide), BF16),
            vmem((line * high, features), BF16),
            vmem((seqs, rows, line * high), BF16),
            vmem((seqs, rows, line * high), BF16),
            vmem((line, rows, width), BF16),
            vmem((line, rows, width), BF16),
            vmem((2, line, chunks, high, wide), BF16),
            vmem((2, line, chunks, high, wide), BF16),
            dma((seqs, chunks)), dma((seqs, chunks)),
            dma((line, HALVES)), dma((line, HALVES)), dma((line, HALVES)),
            dma((line,)), dma((line,)),
            dma((seqs,)), dma((seqs,)),
            dma((seqs,)), dma((seqs,)),
            dma((line,)), dma((line,)),
            dma((2, line, chunks)), dma((2, line, chunks)),
        ],
        compiler_params=pltpu.CompilerParams(collective_id=0, has_side_effects=True),
    )(query, keys, values, upstream, projection, lengths)


def solution(mesh):
    seqs, line = mesh.shape["dp"], mesh.shape["tensor"]

    def shards(query, keys, values, upstream, projection, lengths):
        fits = (
            query.shape[1] == HD
            and projection.shape[0] == HD
            and 1 < seqs
            and 1 < line
            and max(seqs, line) <= MOST_STEPS
            and projection.shape[1] % (CHUNKS * LANES) == 0
            and upstream.shape[0] % (2 * HALVES * 8) == 0
            and upstream.shape[0] * line == query.shape[0]
        )
        if fits:
            return fused_shards(seqs, line, query, keys, values, upstream, projection, lengths)
        return plain_shards(query, keys, values, upstream, projection, lengths)

    in_specs = (
        P(("groups", "dp"), "tensor"),
        P(("groups", "dp"), "tensor"),
        P(("groups", "dp"), "tensor"),
        P(("groups", "dp", "tensor"), None),
        P("tensor", "dp"),
        P(("groups", "dp"), None),
    )
    out_specs = (
        P(("groups", "dp"), "tensor"),
        P(("groups", "dp"), "tensor"),
        P(("groups", "dp"), "tensor"),
        P(("groups", "tensor"), "dp"),
    )
    return jax.shard_map(shards, mesh=mesh, in_specs=in_specs, out_specs=out_specs, check_vma=False)
```

```python
import functools

import jax
import jax.numpy as jnp
from jax import lax
from jax.experimental import pallas as pl
from jax.experimental.pallas import tpu as pltpu
from jax.sharding import PartitionSpec as P

HD = 128
MESH = pl.DeviceIdType.MESH
LANES = 128
CHUNKS = 4
MOST_STEPS = 8
F32 = jnp.float32
BF16 = jnp.bfloat16


def sequence_mask(length_row, row_count):
    segment_ends = jnp.cumsum(length_row)
    places = jnp.arange(row_count, dtype=jnp.int32)
    labels = jnp.sum((segment_ends[None, :] <= places[:, None]).astype(jnp.int32), axis=1)
    same = labels[:, None] == labels[None, :]
    return jnp.logical_and(same, places[None, :] <= places[:, None])


def plain_shards(query, keys, values, upstream, projection, lengths):
    row_count, width = query.shape
    head_count = width // HD
    scaling = HD ** (-0.5)
    allowed = sequence_mask(lengths[0], row_count)
    query_heads = query.reshape(row_count, head_count, HD)
    key_heads = keys.reshape(row_count, head_count, HD)
    value_heads = values.reshape(row_count, head_count, HD)
    scores = (
        jnp.einsum("qhd,khd->hqk", query_heads, key_heads, preferred_element_type=jnp.float32)
        * scaling
    )
    scores = jnp.where(allowed[None], scores, -1e30)
    row_max = jnp.max(scores, axis=2, keepdims=True)
    exponent = jnp.exp(scores - row_max)
    probs = exponent / jnp.sum(exponent, axis=2, keepdims=True)
    probs_low = probs.astype(jnp.bfloat16)
    attended = jnp.einsum(
        "hqk,khd->qhd", probs_low, value_heads, preferred_element_type=jnp.float32
    )
    attended = attended.astype(jnp.bfloat16).reshape(row_count, width)
    full_projection = lax.all_gather(projection, "dp", axis=1, tiled=True)
    gathered = lax.all_gather(upstream, "tensor", axis=0, tiled=True)
    out_total = lax.dot_general(
        gathered, full_projection, (((1,), (1,)), ((), ())), preferred_element_type=jnp.float32
    )
    partial_grad = lax.dot_general(
        attended, gathered, (((0,), (0,)), ((), ())), preferred_element_type=jnp.float32
    )
    grad_projection = lax.psum_scatter(
        partial_grad.astype(jnp.bfloat16), "dp", scatter_dimension=1, tiled=True
    ).astype(jnp.float32)
    out_grad = out_total.astype(jnp.bfloat16)
    grad_heads = out_grad.reshape(row_count, head_count, HD)
    grad_values = jnp.einsum(
        "hqk,qhd->khd", probs_low, grad_heads, preferred_element_type=jnp.float32
    ).astype(jnp.bfloat16)
    grad_probs = jnp.einsum(
        "qhd,khd->hqk", grad_heads, value_heads, preferred_element_type=jnp.float32
    )
    delta = jnp.sum(probs * grad_probs, axis=2, keepdims=True)
    grad_scores = (probs * (grad_probs - delta) * scaling).astype(jnp.bfloat16)
    grad_query = jnp.einsum(
        "hqk,khd->qhd", grad_scores, key_heads, preferred_element_type=jnp.float32
    ).astype(jnp.bfloat16)
    grad_keys = jnp.einsum(
        "hqk,qhd->khd", grad_scores, query_heads, preferred_element_type=jnp.float32
    ).astype(jnp.bfloat16)
    return (
        grad_query.reshape(row_count, width),
        grad_keys.reshape(row_count, width),
        grad_values.reshape(row_count, width),
        grad_projection,
    )


def dot(a, b, over_a, over_b):
    return lax.dot_general(
        a, b, (((over_a,), (over_b,)), ((), ())), preferred_element_type=F32
    )


def kernel(
    seqs, line, chunks,
    query, keys, values, upstream, projection, lengths,
    grad_query, grad_keys, grad_values, grad_projection,
    probs_ref, att_own, att_all, up_all, proj_all, part, part_in, og_own, og_in, stage, landed,
    up_send, up_recv, right_send, left_send, proj_recv, swap_send, swap_recv, att_send, att_recv, spread_send,
    spread_recv, part_send, part_recv, og_send, og_recv, sum_send, sum_recv,
):
    d = lax.axis_index("dp")
    t = lax.axis_index("tensor")
    total = query.shape[0]
    rows, _ = upstream.shape
    high, features = projection.shape
    wide = features // chunks
    half = high // 2
    g = lax.axis_index("groups")
    scaling = HD ** (-0.5)
    pending = []

    def copy(src, dst, send_sem, recv_sem, to_d, to_t):
        return pltpu.make_async_remote_copy(
            src_ref=src, dst_ref=dst, send_sem=send_sem, recv_sem=recv_sem,
            device_id={"dp": to_d, "tensor": to_t}, device_id_type=MESH,
        )

    barrier = pltpu.get_barrier_semaphore()
    for k in range(1, seqs):
        pl.semaphore_signal(
            barrier, inc=1, device_id={"dp": lax.rem(d + k, seqs), "tensor": t},
            device_id_type=MESH,
        )
    for k in range(1, line):
        pl.semaphore_signal(
            barrier, inc=1, device_id={"dp": d, "tensor": lax.rem(t + k, line)},
            device_id_type=MESH,
        )
    pl.semaphore_signal(
        barrier, inc=1, device_id={"groups": 1 - g, "dp": d, "tensor": t}, device_id_type=MESH
    )
    pl.semaphore_wait(barrier, seqs + line - 1)

    others = [lax.rem(d + k, seqs) for k in range(1, seqs)]
    peers = [lax.rem(t + k, line) for k in range(1, line)]
    mine = pl.ds(pl.multiple_of(d * rows, rows), rows)
    right = jnp.minimum(t + 1, line - 1)
    left = jnp.maximum(t - 1, 0)

    def send_upstream(c):
        for o in others:
            off = pl.multiple_of(o * features + c * wide, wide)
            one = copy(
                upstream.at[:, pl.ds(off, wide)], up_all.at[c, mine],
                up_send.at[o, c], up_recv.at[d, c], o, t,
            )
            one.start()
            pending.append((None, one))

    waited = set()

    def wait_upstream(c):
        if c in waited:
            return
        waited.add(c)
        for o in others:
            dst = up_all.at[c, pl.ds(pl.multiple_of(o * rows, rows), rows)]
            copy(dst, dst, up_send.at[o, c], up_recv.at[o, c], o, t).wait_recv()

    def block(j, p):
        return proj_all.at[pl.ds(pl.multiple_of(j * high + p * half, half), half)]

    def proj_send(j, source, where, toward):
        sems = right_send if toward is right else left_send
        one = copy(source, block(j, g), sems.at[j], proj_recv.at[j], d, toward)

        @pl.when(where)
        def _():
            one.start()

        pending.append((where, one))

    def proj_own():
        source = projection.at[pl.ds(pl.multiple_of(g * half, half), half)]
        proj_send(t, source, t < line - 1, right)
        proj_send(t, source, t > 0, left)

    def swap(j, p):
        return pltpu.make_async_remote_copy(
            src_ref=block(j, p), dst_ref=block(j, p), send_sem=swap_send.at[j],
            recv_sem=swap_recv.at[j], device_id={"groups": 1 - g, "dp": d, "tensor": t},
            device_id_type=MESH,
        )

    def proj_step(k):
        from_left, from_right = jnp.maximum(t - k, 0), jnp.minimum(t + k, line - 1)
        for j, here, toward, on in (
            (from_left, t >= k, right, t < line - 1),
            (from_right, t + k < line, left, t > 0),
        ):
            dst = block(j, g)
            across = swap(j, g)

            @pl.when(here)
            def _(dst=dst, j=j, across=across):
                copy(dst, dst, right_send.at[j], proj_recv.at[j], d, right).wait_recv()
                across.start()

            pending.append((here, across))
            if k < line - 1:
                proj_send(j, dst, jnp.logical_and(here, on), toward)

    def wait_swaps():
        for j in peers:
            swap(j, 1 - g).wait_recv()

    early = max(1, chunks // 4)
    for c in range(early):
        send_upstream(c)

    ends = []
    sofar = lengths[0, 0]
    for n in range(lengths.shape[1]):
        ends.append(sofar)
        if n + 1 < lengths.shape[1]:
            sofar = sofar + lengths[0, n + 1]
    down = lax.broadcasted_iota(jnp.int32, (total, 1), 0)
    across = lax.broadcasted_iota(jnp.int32, (1, total), 1)
    label_down = sum((down >= e).astype(jnp.int32) for e in ends)
    label_across = sum((across >= e).astype(jnp.int32) for e in ends)
    for q in range(line):
        span = slice(q * rows, (q + 1) * rows)
        scores = dot(query[span, :], keys[...], 1, 1) * scaling
        allowed = jnp.logical_and(label_down[span] == label_across, across <= down[span])
        scores = jnp.where(allowed, scores, -1e30)
        exponent = jnp.exp(scores - jnp.max(scores, axis=1, keepdims=True))
        probs = exponent / jnp.sum(exponent, axis=1, keepdims=True)
        probs_ref[span, :] = probs
        att_own[q] = dot(probs.astype(BF16), values[...], 1, 0).astype(BF16)
    att_all[t, mine] = att_own[t]
    for o in peers:
        one = copy(
            att_own.at[o], att_all.at[t, mine], att_send.at[o], att_recv.at[t], d, o
        )
        one.start()
        pending.append((None, one))
    proj_own()
    for c in range(chunks):
        up_all[c, mine] = upstream[:, pl.ds(pl.multiple_of(d * features + c * wide, wide), wide)]
    proj_all[pl.ds(pl.multiple_of(t * high, high), high), :] = projection[...]
    for o in peers:
        dst = att_all.at[o, mine]
        copy(dst, dst, att_send.at[o], att_recv.at[o], d, o).wait_recv()
    for o in others:
        one = copy(
            att_all.at[:, mine], att_all.at[:, mine], spread_send.at[o], spread_recv.at[d], o, t
        )
        one.start()
        pending.append((None, one))
    for c in range(early, chunks):
        send_upstream(c)
    proj_step(1)
    for o in others:
        dst = att_all.at[:, pl.ds(pl.multiple_of(o * rows, rows), rows)]
        copy(dst, dst, spread_send.at[o], spread_recv.at[o], o, t).wait_recv()

    def sum_chunk(c):
        wait_upstream(c)
        for k in range(line - 1, 0, -1):
            for way, head, go, first, toward in (
                (0, jnp.minimum(t + k, line - 1), t + k < line, t == 0, right),
                (1, jnp.maximum(t - k, 0), t >= k, t == line - 1, left),
            ):
                one = copy(
                    stage.at[way, head, c], landed.at[way, head, c],
                    sum_send.at[way, head, c], sum_recv.at[way, head, c], d, toward,
                )

                @pl.when(go)
                def _(way=way, head=head, first=first, one=one):
                    term = dot(att_all[head], up_all[c], 0, 0)

                    @pl.when(first)
                    def _():
                        stage[way, head, c] = term.astype(BF16)

                    @pl.when(jnp.logical_not(first))
                    def _():
                        one.wait_recv()
                        stage[way, head, c] = (
                            term + landed[way, head, c].astype(F32)
                        ).astype(BF16)

                    one.start()

                pending.append((go, one))

    def own_term(c):
        cols = slice(c * wide, (c + 1) * wide)
        grad_projection[:, cols] = dot(att_all[t], up_all[c], 0, 0)

    def own_chunk(c):
        cols = slice(c * wide, (c + 1) * wide)
        for way, there in ((0, t > 0), (1, t < line - 1)):
            dst = landed.at[way, t, c]

            @pl.when(there)
            def _(way=way, dst=dst):
                copy(
                    dst, dst, sum_send.at[way, t, c], sum_recv.at[way, t, c], d, right
                ).wait_recv()
                grad_projection[:, cols] += landed[way, t, c].astype(F32)

    def part_copy(o):
        return copy(part.at[o], part_in.at[d], part_send.at[o], part_recv.at[d], o, t)

    def out_partials():
        wait_swaps()
        for o in others + [d]:
            at = pl.ds(pl.multiple_of(o * rows, rows), rows)
            piece = dot(up_all[0, at], proj_all[:, :wide], 1, 1)
            for c in range(1, chunks):
                piece += dot(up_all[c, at], proj_all[:, c * wide:(c + 1) * wide], 1, 1)
            if o is d:
                part_in[d] = piece.astype(BF16)
                continue
            part[o] = piece.astype(BF16)
            part_copy(o).start()

    def out_sum():
        for o in others:
            pending.append((None, part_copy(o)))
            dst = part_in.at[o]
            copy(dst, dst, part_send.at[o], part_recv.at[o], o, t).wait_recv()
        whole = sum(part_in[n].astype(F32) for n in range(seqs)).astype(BF16)
        for q in range(line):
            og_own[q] = whole[:, q * HD:(q + 1) * HD]
        og_in[t] = og_own[t]
        for o in peers:
            one = copy(og_own.at[o], og_in.at[t], og_send.at[o], og_recv.at[t], d, o)
            one.start()
            pending.append((None, one))

    inner = jnp.logical_and(t > 0, t < line - 1)
    for c in range(chunks):
        if c == chunks // 2:
            for later in range(c, chunks):
                wait_upstream(later)

            @pl.when(inner)
            def _():
                out_partials()

        if c == chunks - 1:

            @pl.when(jnp.logical_not(inner))
            def _():
                out_partials()

            out_sum()
        sum_chunk(c)
        if c < line - 2:
            proj_step(c + 2)
    for c in range(chunks):
        own_term(c)

    for o in peers:
        dst = og_in.at[o]
        copy(dst, dst, og_send.at[o], og_recv.at[o], d, o).wait_recv()
    grads = [og_in[q] for q in range(line)]
    gv = 0.0
    gk = 0.0
    for q in range(line):
        span = slice(q * rows, (q + 1) * rows)
        probs = probs_ref[span, :]
        gv = gv + dot(probs.astype(BF16), grads[q], 0, 0)
        grad_probs = dot(grads[q], values[...], 1, 1)
        delta = jnp.sum(probs * grad_probs, axis=1, keepdims=True)
        grad_scores = (probs * (grad_probs - delta) * scaling).astype(BF16)
        grad_query[span, :] = dot(grad_scores, keys[...], 1, 0).astype(BF16)
        gk = gk + dot(grad_scores, query[span, :], 0, 0)
    grad_values[...] = gv.astype(BF16)
    grad_keys[...] = gk.astype(BF16)
    for c in range(chunks):
        own_chunk(c)

    for where, one in pending:
        if where is None:
            one.wait_send()
        else:

            @pl.when(where)
            def _(one=one):
                one.wait_send()


def hand_on(pieces, *refs):
    count = (len(refs) - 2) // 3
    ins, outs, held = refs[:count], refs[count:2 * count], refs[2 * count:3 * count]
    in_sems, out_sems = refs[3 * count:]
    steps = []
    for n, (i, o, h) in enumerate(zip(ins, outs, held)):
        size = i.shape[0] // pieces
        for p in range(pieces):
            at = pl.ds(p * size, size)
            steps.append((
                pltpu.make_async_copy(i.at[at], h.at[at], in_sems.at[n, p]),
                pltpu.make_async_copy(h.at[at], o.at[at], out_sems.at[n, p]),
            ))
    for take, _ in steps:
        take.start()
    for take, give in steps:
        take.wait()
        give.start()
    for _, give in steps:
        give.wait()


def handed_on(arrays, pieces=2):
    held = pl.BlockSpec(memory_space=pl.ANY)
    return pl.pallas_call(
        functools.partial(hand_on, pieces),
        out_shape=tuple(jax.ShapeDtypeStruct(a.shape, a.dtype) for a in arrays),
        in_specs=[held] * len(arrays),
        out_specs=(held,) * len(arrays),
        scratch_shapes=[pltpu.VMEM(a.shape, a.dtype) for a in arrays]
        + [pltpu.SemaphoreType.DMA((len(arrays), pieces))] * 2,
    )(*arrays)


def fused_shards(seqs, line, query, keys, values, upstream, projection, lengths):
    total, width = query.shape
    rows = upstream.shape[0]
    high, features = projection.shape
    chunks = CHUNKS
    wide = features // chunks
    dma = pltpu.SemaphoreType.DMA
    vmem = pltpu.VMEM
    whole = pl.BlockSpec(memory_space=pltpu.VMEM)
    grads = pl.pallas_call(
        functools.partial(kernel, seqs, line, chunks),
        out_shape=(
            jax.ShapeDtypeStruct(query.shape, BF16),
            jax.ShapeDtypeStruct(query.shape, BF16),
            jax.ShapeDtypeStruct(query.shape, BF16),
            jax.ShapeDtypeStruct(projection.shape, F32),
        ),
        in_specs=[whole] * 5 + [pl.BlockSpec(memory_space=pltpu.SMEM)],
        out_specs=(whole,) * 4,
        scratch_shapes=[
            vmem((total, total), F32),
            vmem((line, rows, width), BF16),
            vmem((line, seqs * rows, width), BF16),
            vmem((chunks, seqs * rows, wide), BF16),
            vmem((line * high, features), BF16),
            vmem((seqs, rows, line * high), BF16),
            vmem((seqs, rows, line * high), BF16),
            vmem((line, rows, width), BF16),
            vmem((line, rows, width), BF16),
            vmem((2, line, chunks, high, wide), BF16),
            vmem((2, line, chunks, high, wide), BF16),
            dma((seqs, chunks)), dma((seqs, chunks)),
            dma((line,)), dma((line,)), dma((line,)), dma((line,)), dma((line,)),
            dma((line,)), dma((line,)),
            dma((seqs,)), dma((seqs,)),
            dma((seqs,)), dma((seqs,)),
            dma((line,)), dma((line,)),
            dma((2, line, chunks)), dma((2, line, chunks)),
        ],
        compiler_params=pltpu.CompilerParams(collective_id=0, has_side_effects=True),
    )(query, keys, values, upstream, projection, lengths)
    return handed_on(grads)


def solution(mesh):
    seqs, line = mesh.shape["dp"], mesh.shape["tensor"]

    def shards(query, keys, values, upstream, projection, lengths):
        fits = (
            query.shape[1] == HD
            and projection.shape[0] == HD
            and 1 < seqs
            and 1 < line
            and max(seqs, line) <= MOST_STEPS
            and projection.shape[1] % (CHUNKS * LANES) == 0
            and upstream.shape[0] % 32 == 0
            and mesh.shape["groups"] == 2
            and line - 2 <= CHUNKS // 2
            and upstream.shape[0] * line == query.shape[0]
        )
        if fits:
            return fused_shards(seqs, line, query, keys, values, upstream, projection, lengths)
        return plain_shards(query, keys, values, upstream, projection, lengths)

    in_specs = (
        P(("groups", "dp"), "tensor"),
        P(("groups", "dp"), "tensor"),
        P(("groups", "dp"), "tensor"),
        P(("groups", "dp", "tensor"), None),
        P("tensor", "dp"),
        P(("groups", "dp"), None),
    )
    out_specs = (
        P(("groups", "dp"), "tensor"),
        P(("groups", "dp"), "tensor"),
        P(("groups", "dp"), "tensor"),
        P(("groups", "tensor"), "dp"),
    )
    return jax.shard_map(shards, mesh=mesh, in_specs=in_specs, out_specs=out_specs, check_vma=False)
```

```python
import functools

import jax
import jax.numpy as jnp
from jax import lax
from jax.experimental import pallas as pl
from jax.experimental.pallas import tpu as pltpu
from jax.sharding import PartitionSpec as P

HD = 128
MESH = pl.DeviceIdType.MESH
LANES = 128
CHUNKS = 4
MOST_STEPS = 8
F32 = jnp.float32
BF16 = jnp.bfloat16


def sequence_mask(length_row, row_count):
    segment_ends = jnp.cumsum(length_row)
    places = jnp.arange(row_count, dtype=jnp.int32)
    labels = jnp.sum((segment_ends[None, :] <= places[:, None]).astype(jnp.int32), axis=1)
    same = labels[:, None] == labels[None, :]
    return jnp.logical_and(same, places[None, :] <= places[:, None])


def plain_shards(query, keys, values, upstream, projection, lengths):
    row_count, width = query.shape
    head_count = width // HD
    scaling = HD ** (-0.5)
    allowed = sequence_mask(lengths[0], row_count)
    query_heads = query.reshape(row_count, head_count, HD)
    key_heads = keys.reshape(row_count, head_count, HD)
    value_heads = values.reshape(row_count, head_count, HD)
    scores = (
        jnp.einsum("qhd,khd->hqk", query_heads, key_heads, preferred_element_type=jnp.float32)
        * scaling
    )
    scores = jnp.where(allowed[None], scores, -1e30)
    row_max = jnp.max(scores, axis=2, keepdims=True)
    exponent = jnp.exp(scores - row_max)
    probs = exponent / jnp.sum(exponent, axis=2, keepdims=True)
    probs_low = probs.astype(jnp.bfloat16)
    attended = jnp.einsum(
        "hqk,khd->qhd", probs_low, value_heads, preferred_element_type=jnp.float32
    )
    attended = attended.astype(jnp.bfloat16).reshape(row_count, width)
    full_projection = lax.all_gather(projection, "dp", axis=1, tiled=True)
    gathered = lax.all_gather(upstream, "tensor", axis=0, tiled=True)
    out_total = lax.dot_general(
        gathered, full_projection, (((1,), (1,)), ((), ())), preferred_element_type=jnp.float32
    )
    partial_grad = lax.dot_general(
        attended, gathered, (((0,), (0,)), ((), ())), preferred_element_type=jnp.float32
    )
    grad_projection = lax.psum_scatter(
        partial_grad.astype(jnp.bfloat16), "dp", scatter_dimension=1, tiled=True
    ).astype(jnp.float32)
    out_grad = out_total.astype(jnp.bfloat16)
    grad_heads = out_grad.reshape(row_count, head_count, HD)
    grad_values = jnp.einsum(
        "hqk,qhd->khd", probs_low, grad_heads, preferred_element_type=jnp.float32
    ).astype(jnp.bfloat16)
    grad_probs = jnp.einsum(
        "qhd,khd->hqk", grad_heads, value_heads, preferred_element_type=jnp.float32
    )
    delta = jnp.sum(probs * grad_probs, axis=2, keepdims=True)
    grad_scores = (probs * (grad_probs - delta) * scaling).astype(jnp.bfloat16)
    grad_query = jnp.einsum(
        "hqk,khd->qhd", grad_scores, key_heads, preferred_element_type=jnp.float32
    ).astype(jnp.bfloat16)
    grad_keys = jnp.einsum(
        "hqk,qhd->khd", grad_scores, query_heads, preferred_element_type=jnp.float32
    ).astype(jnp.bfloat16)
    return (
        grad_query.reshape(row_count, width),
        grad_keys.reshape(row_count, width),
        grad_values.reshape(row_count, width),
        grad_projection,
    )


def dot(a, b, over_a, over_b):
    return lax.dot_general(
        a, b, (((over_a,), (over_b,)), ((), ())), preferred_element_type=F32
    )


def kernel(
    seqs, line, chunks,
    query, keys, values, upstream, projection, lengths,
    grad_query, grad_keys, grad_values, grad_projection,
    probs_ref, att_own, att_all, att_turned, out_acc, up_all, proj_all, part, part_in, og_own, og_in, stage, landed,
    up_send, up_recv, right_send, left_send, proj_recv, swap_send, swap_recv, att_send, att_recv, spread_send,
    spread_recv, part_send, part_recv, og_send, og_recv, sum_send, sum_recv,
):
    d = lax.axis_index("dp")
    t = lax.axis_index("tensor")
    total = query.shape[0]
    rows, _ = upstream.shape
    high, features = projection.shape
    wide = features // chunks
    half = high // 2
    g = lax.axis_index("groups")
    scaling = HD ** (-0.5)
    pending = []

    def copy(src, dst, send_sem, recv_sem, to_d, to_t):
        return pltpu.make_async_remote_copy(
            src_ref=src, dst_ref=dst, send_sem=send_sem, recv_sem=recv_sem,
            device_id={"dp": to_d, "tensor": to_t}, device_id_type=MESH,
        )

    barrier = pltpu.get_barrier_semaphore()
    for k in range(1, seqs):
        pl.semaphore_signal(
            barrier, inc=1, device_id={"dp": lax.rem(d + k, seqs), "tensor": t},
            device_id_type=MESH,
        )
    for k in range(1, line):
        pl.semaphore_signal(
            barrier, inc=1, device_id={"dp": d, "tensor": lax.rem(t + k, line)},
            device_id_type=MESH,
        )
    pl.semaphore_signal(
        barrier, inc=1, device_id={"groups": 1 - g, "dp": d, "tensor": t}, device_id_type=MESH
    )
    pl.semaphore_wait(barrier, seqs + line - 1)

    others = [lax.rem(d + k, seqs) for k in range(1, seqs)]
    peers = [lax.rem(t + k, line) for k in range(1, line)]
    mine = pl.ds(pl.multiple_of(d * rows, rows), rows)
    right = jnp.minimum(t + 1, line - 1)
    left = jnp.maximum(t - 1, 0)

    def send_upstream(c):
        for o in others:
            off = pl.multiple_of(o * features + c * wide, wide)
            one = copy(
                upstream.at[:, pl.ds(off, wide)], up_all.at[c, mine],
                up_send.at[o, c], up_recv.at[d, c], o, t,
            )
            one.start()
            pending.append((None, one))

    def wait_upstream(c):
        for o in others:
            dst = up_all.at[c, pl.ds(pl.multiple_of(o * rows, rows), rows)]
            copy(dst, dst, up_send.at[o, c], up_recv.at[o, c], o, t).wait_recv()

    def block(j, p):
        return proj_all.at[pl.ds(pl.multiple_of(j * high + p * half, half), half)]

    def proj_send(j, source, where, toward, run=True, keep=True):
        sems = right_send if toward is right else left_send
        one = copy(source, block(j, g), sems.at[j], proj_recv.at[j], d, toward)
        if run:

            @pl.when(where)
            def _():
                one.start()

        if keep:
            pending.append((where, one))

    def proj_own():
        source = projection.at[pl.ds(pl.multiple_of(g * half, half), half)]
        proj_send(t, source, t < line - 1, right)
        proj_send(t, source, t > 0, left)

    def swap(j, p):
        return pltpu.make_async_remote_copy(
            src_ref=block(j, p), dst_ref=block(j, p), send_sem=swap_send.at[j],
            recv_sem=swap_recv.at[j], device_id={"groups": 1 - g, "dp": d, "tensor": t},
            device_id_type=MESH,
        )

    def proj_step(k, run=True):
        from_left, from_right = jnp.maximum(t - k, 0), jnp.minimum(t + k, line - 1)
        for j, here, toward, on in (
            (from_left, t >= k, right, t < line - 1),
            (from_right, t + k < line, left, t > 0),
        ):
            dst = block(j, g)
            across = swap(j, g)
            if not run:
                pending.append((here, across))
            else:

                @pl.when(here)
                def _(dst=dst, j=j, across=across):
                    copy(dst, dst, right_send.at[j], proj_recv.at[j], d, right).wait_recv()
                    across.start()

            if k < line - 1:
                proj_send(j, dst, jnp.logical_and(here, on), toward, run, not run)

    def wait_swaps():
        for j in peers:
            swap(j, 1 - g).wait_recv()

    early = max(1, chunks // 4)
    for c in range(early):
        send_upstream(c)
    proj_own()

    ends = []
    sofar = lengths[0, 0]
    for n in range(lengths.shape[1]):
        ends.append(sofar)
        if n + 1 < lengths.shape[1]:
            sofar = sofar + lengths[0, n + 1]
    down = lax.broadcasted_iota(jnp.int32, (total, 1), 0)
    across = lax.broadcasted_iota(jnp.int32, (1, total), 1)
    label_down = sum((down >= e).astype(jnp.int32) for e in ends)
    label_across = sum((across >= e).astype(jnp.int32) for e in ends)
    for q in range(line):
        span = slice(q * rows, (q + 1) * rows)
        scores = dot(query[span, :], keys[...], 1, 1) * scaling
        allowed = jnp.logical_and(label_down[span] == label_across, across <= down[span])
        scores = jnp.where(allowed, scores, -1e30)
        exponent = jnp.exp(scores - jnp.max(scores, axis=1, keepdims=True))
        probs = exponent / jnp.sum(exponent, axis=1, keepdims=True)
        probs_ref[span, :] = probs
        att_own[q] = dot(probs.astype(BF16), values[...], 1, 0).astype(BF16)
    att_all[t, mine] = att_own[t]
    for o in peers:
        one = copy(
            att_own.at[o], att_all.at[t, mine], att_send.at[o], att_recv.at[t], d, o
        )
        one.start()
        pending.append((None, one))
    for c in range(chunks):
        up_all[c, mine] = upstream[:, pl.ds(pl.multiple_of(d * features + c * wide, wide), wide)]
    proj_all[pl.ds(pl.multiple_of(t * high, high), high), :] = projection[...]
    for o in peers:
        dst = att_all.at[o, mine]
        copy(dst, dst, att_send.at[o], att_recv.at[o], d, o).wait_recv()
    for o in others:
        one = copy(
            att_all.at[:, mine], att_all.at[:, mine], spread_send.at[o], spread_recv.at[d], o, t
        )
        one.start()
        pending.append((None, one))
    for c in range(early, chunks):
        send_upstream(c)
    proj_step(1)
    for o in others:
        dst = att_all.at[:, pl.ds(pl.multiple_of(o * rows, rows), rows)]
        copy(dst, dst, spread_send.at[o], spread_recv.at[o], o, t).wait_recv()

    def sum_chunk(c, run=True):
        for k in range(line - 1, 0, -1):
            for way, head, go, first, toward in (
                (0, jnp.minimum(t + k, line - 1), t + k < line, t == 0, right),
                (1, jnp.maximum(t - k, 0), t >= k, t == line - 1, left),
            ):
                one = copy(
                    stage.at[way, head, c], landed.at[way, head, c],
                    sum_send.at[way, head, c], sum_recv.at[way, head, c], d, toward,
                )

                if not run:
                    pending.append((go, one))
                    continue

                @pl.when(go)
                def _(way=way, head=head, first=first, one=one):
                    if c == 0:
                        att_turned[head] = att_all[head].T
                    term = dot(att_turned[head], up_all[c], 1, 0)

                    @pl.when(first)
                    def _():
                        stage[way, head, c] = term.astype(BF16)

                    @pl.when(jnp.logical_not(first))
                    def _():
                        one.wait_recv()
                        stage[way, head, c] = (
                            term + landed[way, head, c].astype(F32)
                        ).astype(BF16)

                    one.start()


    def own_term(c):
        cols = slice(c * wide, (c + 1) * wide)
        if c == 0:
            att_turned[t] = att_all[t].T
        grad_projection[:, cols] = dot(att_turned[t], up_all[c], 1, 0)

    def own_chunk(c):
        cols = slice(c * wide, (c + 1) * wide)
        for way, there in ((0, t > 0), (1, t < line - 1)):
            dst = landed.at[way, t, c]

            @pl.when(there)
            def _(way=way, dst=dst):
                copy(
                    dst, dst, sum_send.at[way, t, c], sum_recv.at[way, t, c], d, right
                ).wait_recv()
                grad_projection[:, cols] += landed[way, t, c].astype(F32)

    def part_copy(o):
        return copy(part.at[o], part_in.at[d], part_send.at[o], part_recv.at[d], o, t)

    def out_term(c):
        piece = dot(up_all[c], proj_all[:, c * wide:(c + 1) * wide], 1, 1)
        if c == 0:
            out_acc[...] = piece
        else:
            out_acc[...] += piece

    def out_partials():
        for o in others + [d]:
            at = pl.ds(pl.multiple_of(o * rows, rows), rows)
            if o is d:
                part_in[d] = out_acc[at, :].astype(BF16)
                continue
            part[o] = out_acc[at, :].astype(BF16)
            part_copy(o).start()

    def out_sum():
        for o in others:
            pending.append((None, part_copy(o)))
            dst = part_in.at[o]
            copy(dst, dst, part_send.at[o], part_recv.at[o], o, t).wait_recv()
        whole = sum(part_in[n].astype(F32) for n in range(seqs)).astype(BF16)
        for q in range(line):
            og_own[q] = whole[:, q * HD:(q + 1) * HD]
        og_in[t] = og_own[t]
        for o in peers:
            one = copy(og_own.at[o], og_in.at[t], og_send.at[o], og_recv.at[t], d, o)
            one.start()
            pending.append((None, one))

    inner = jnp.logical_and(t > 0, t < line - 1)
    outer = jnp.logical_not(inner)
    wait_upstream(0)
    for k in range(2, line - 1):

        @pl.when(inner)
        def _(k=k):
            proj_step(k)

    sum_chunk(0)
    for k in range(2, line - 1):

        @pl.when(outer)
        def _(k=k):
            proj_step(k)

    wait_upstream(1)
    sum_chunk(1)
    proj_step(line - 1)
    wait_swaps()
    out_term(0)
    out_term(1)
    for c in range(2, chunks - 1):
        wait_upstream(c)
        out_term(c)

        @pl.when(outer)
        def _(c=c):
            sum_chunk(c)

    wait_upstream(chunks - 1)
    out_term(chunks - 1)
    out_partials()
    for c in range(2, chunks - 1):

        @pl.when(inner)
        def _(c=c):
            sum_chunk(c)

    for c in range(chunks - 1):
        own_term(c)
    out_sum()
    sum_chunk(chunks - 1)
    own_term(chunks - 1)

    for o in peers:
        dst = og_in.at[o]
        copy(dst, dst, og_send.at[o], og_recv.at[o], d, o).wait_recv()
    grads = [og_in[q] for q in range(line)]
    gv = 0.0
    gk = 0.0
    for q in range(line):
        span = slice(q * rows, (q + 1) * rows)
        probs = probs_ref[span, :]
        gv = gv + dot(probs.astype(BF16), grads[q], 0, 0)
        grad_probs = dot(grads[q], values[...], 1, 1)
        delta = jnp.sum(probs * grad_probs, axis=1, keepdims=True)
        grad_scores = (probs * (grad_probs - delta) * scaling).astype(BF16)
        grad_query[span, :] = dot(grad_scores, keys[...], 1, 0).astype(BF16)
        gk = gk + dot(grad_scores, query[span, :], 0, 0)
    grad_values[...] = gv.astype(BF16)
    grad_keys[...] = gk.astype(BF16)
    for c in range(chunks):
        own_chunk(c)

    for k in range(1, line):
        proj_step(k, False)
    for c in range(chunks):
        sum_chunk(c, False)
    for where, one in pending:
        if where is None:
            one.wait_send()
        else:

            @pl.when(where)
            def _(one=one):
                one.wait_send()


def hand_on(pieces, *refs):
    count = (len(refs) - 2) // 3
    ins, outs, held = refs[:count], refs[count:2 * count], refs[2 * count:3 * count]
    in_sems, out_sems = refs[3 * count:]
    steps = []
    for n, (i, o, h) in enumerate(zip(ins, outs, held)):
        size = i.shape[0] // pieces
        for p in range(pieces):
            at = pl.ds(p * size, size)
            steps.append((
                pltpu.make_async_copy(i.at[at], h.at[at], in_sems.at[n, p]),
                pltpu.make_async_copy(h.at[at], o.at[at], out_sems.at[n, p]),
            ))
    for take, _ in steps:
        take.start()
    for take, give in steps:
        take.wait()
        give.start()
    for _, give in steps:
        give.wait()


def handed_on(arrays, pieces=2):
    held = pl.BlockSpec(memory_space=pl.ANY)
    return pl.pallas_call(
        functools.partial(hand_on, pieces),
        out_shape=tuple(jax.ShapeDtypeStruct(a.shape, a.dtype) for a in arrays),
        in_specs=[held] * len(arrays),
        out_specs=(held,) * len(arrays),
        scratch_shapes=[pltpu.VMEM(a.shape, a.dtype) for a in arrays]
        + [pltpu.SemaphoreType.DMA((len(arrays), pieces))] * 2,
    )(*arrays)


def fused_shards(seqs, line, query, keys, values, upstream, projection, lengths):
    total, width = query.shape
    rows = upstream.shape[0]
    high, features = projection.shape
    chunks = CHUNKS
    wide = features // chunks
    dma = pltpu.SemaphoreType.DMA
    vmem = pltpu.VMEM
    whole = pl.BlockSpec(memory_space=pltpu.VMEM)
    grads = pl.pallas_call(
        functools.partial(kernel, seqs, line, chunks),
        out_shape=(
            jax.ShapeDtypeStruct(query.shape, BF16),
            jax.ShapeDtypeStruct(query.shape, BF16),
            jax.ShapeDtypeStruct(query.shape, BF16),
            jax.ShapeDtypeStruct(projection.shape, F32),
        ),
        in_specs=[whole] * 5 + [pl.BlockSpec(memory_space=pltpu.SMEM)],
        out_specs=(whole,) * 4,
        scratch_shapes=[
            vmem((total, total), F32),
            vmem((line, rows, width), BF16),
            vmem((line, seqs * rows, width), BF16),
            vmem((line, width, seqs * rows), BF16),
            vmem((seqs * rows, line * high), F32),
            vmem((chunks, seqs * rows, wide), BF16),
            vmem((line * high, features), BF16),
            vmem((seqs, rows, line * high), BF16),
            vmem((seqs, rows, line * high), BF16),
            vmem((line, rows, width), BF16),
            vmem((line, rows, width), BF16),
            vmem((2, line, chunks, high, wide), BF16),
            vmem((2, line, chunks, high, wide), BF16),
            dma((seqs, chunks)), dma((seqs, chunks)),
            dma((line,)), dma((line,)), dma((line,)), dma((line,)), dma((line,)),
            dma((line,)), dma((line,)),
            dma((seqs,)), dma((seqs,)),
            dma((seqs,)), dma((seqs,)),
            dma((line,)), dma((line,)),
            dma((2, line, chunks)), dma((2, line, chunks)),
        ],
        compiler_params=pltpu.CompilerParams(collective_id=0, has_side_effects=True),
    )(query, keys, values, upstream, projection, lengths)
    return handed_on(grads)


def solution(mesh):
    seqs, line = mesh.shape["dp"], mesh.shape["tensor"]

    def shards(query, keys, values, upstream, projection, lengths):
        fits = (
            query.shape[1] == HD
            and projection.shape[0] == HD
            and 1 < seqs
            and 1 < line
            and max(seqs, line) <= MOST_STEPS
            and projection.shape[1] % (CHUNKS * LANES) == 0
            and upstream.shape[0] % 32 == 0
            and mesh.shape["groups"] == 2
            and 3 <= line
            and upstream.shape[0] * line == query.shape[0]
        )
        if fits:
            return fused_shards(seqs, line, query, keys, values, upstream, projection, lengths)
        return plain_shards(query, keys, values, upstream, projection, lengths)

    in_specs = (
        P(("groups", "dp"), "tensor"),
        P(("groups", "dp"), "tensor"),
        P(("groups", "dp"), "tensor"),
        P(("groups", "dp", "tensor"), None),
        P("tensor", "dp"),
        P(("groups", "dp"), None),
    )
    out_specs = (
        P(("groups", "dp"), "tensor"),
        P(("groups", "dp"), "tensor"),
        P(("groups", "dp"), "tensor"),
        P(("groups", "tensor"), "dp"),
    )
    return jax.shard_map(shards, mesh=mesh, in_specs=in_specs, out_specs=out_specs, check_vma=False)
```

```python
import functools

import jax
import jax.numpy as jnp
from jax import lax
from jax.experimental import pallas as pl
from jax.experimental.pallas import tpu as pltpu
from jax.sharding import PartitionSpec as P

HD = 128
MESH = pl.DeviceIdType.MESH
LANES = 128
CHUNKS = 4
MOST_STEPS = 8
F32 = jnp.float32
BF16 = jnp.bfloat16


def sequence_mask(length_row, row_count):
    segment_ends = jnp.cumsum(length_row)
    places = jnp.arange(row_count, dtype=jnp.int32)
    labels = jnp.sum((segment_ends[None, :] <= places[:, None]).astype(jnp.int32), axis=1)
    same = labels[:, None] == labels[None, :]
    return jnp.logical_and(same, places[None, :] <= places[:, None])


def plain_shards(query, keys, values, upstream, projection, lengths):
    row_count, width = query.shape
    head_count = width // HD
    scaling = HD ** (-0.5)
    allowed = sequence_mask(lengths[0], row_count)
    query_heads = query.reshape(row_count, head_count, HD)
    key_heads = keys.reshape(row_count, head_count, HD)
    value_heads = values.reshape(row_count, head_count, HD)
    scores = (
        jnp.einsum("qhd,khd->hqk", query_heads, key_heads, preferred_element_type=jnp.float32)
        * scaling
    )
    scores = jnp.where(allowed[None], scores, -1e30)
    row_max = jnp.max(scores, axis=2, keepdims=True)
    exponent = jnp.exp(scores - row_max)
    probs = exponent / jnp.sum(exponent, axis=2, keepdims=True)
    probs_low = probs.astype(jnp.bfloat16)
    attended = jnp.einsum(
        "hqk,khd->qhd", probs_low, value_heads, preferred_element_type=jnp.float32
    )
    attended = attended.astype(jnp.bfloat16).reshape(row_count, width)
    full_projection = lax.all_gather(projection, "dp", axis=1, tiled=True)
    gathered = lax.all_gather(upstream, "tensor", axis=0, tiled=True)
    out_total = lax.dot_general(
        gathered, full_projection, (((1,), (1,)), ((), ())), preferred_element_type=jnp.float32
    )
    partial_grad = lax.dot_general(
        attended, gathered, (((0,), (0,)), ((), ())), preferred_element_type=jnp.float32
    )
    grad_projection = lax.psum_scatter(
        partial_grad.astype(jnp.bfloat16), "dp", scatter_dimension=1, tiled=True
    ).astype(jnp.float32)
    out_grad = out_total.astype(jnp.bfloat16)
    grad_heads = out_grad.reshape(row_count, head_count, HD)
    grad_values = jnp.einsum(
        "hqk,qhd->khd", probs_low, grad_heads, preferred_element_type=jnp.float32
    ).astype(jnp.bfloat16)
    grad_probs = jnp.einsum(
        "qhd,khd->hqk", grad_heads, value_heads, preferred_element_type=jnp.float32
    )
    delta = jnp.sum(probs * grad_probs, axis=2, keepdims=True)
    grad_scores = (probs * (grad_probs - delta) * scaling).astype(jnp.bfloat16)
    grad_query = jnp.einsum(
        "hqk,khd->qhd", grad_scores, key_heads, preferred_element_type=jnp.float32
    ).astype(jnp.bfloat16)
    grad_keys = jnp.einsum(
        "hqk,qhd->khd", grad_scores, query_heads, preferred_element_type=jnp.float32
    ).astype(jnp.bfloat16)
    return (
        grad_query.reshape(row_count, width),
        grad_keys.reshape(row_count, width),
        grad_values.reshape(row_count, width),
        grad_projection,
    )


def dot(a, b, over_a, over_b):
    return lax.dot_general(
        a, b, (((over_a,), (over_b,)), ((), ())), preferred_element_type=F32
    )


def kernel(
    seqs, line, chunks,
    query, keys, values, upstream, projection, lengths,
    grad_query, grad_keys, grad_values, grad_projection,
    probs_ref, att_own, att_all, att_turned, out_acc, up_all, proj_all, part, part_in, og_own, og_in, stage, landed,
    up_send, up_recv, right_send, left_send, proj_recv, swap_send, swap_recv, att_send, att_recv, spread_send,
    spread_recv, part_send, part_recv, og_send, og_recv, sum_send, sum_recv,
):
    d = lax.axis_index("dp")
    t = lax.axis_index("tensor")
    total = query.shape[0]
    rows, _ = upstream.shape
    high, features = projection.shape
    wide = features // chunks
    half = high // 2
    g = lax.axis_index("groups")
    scaling = HD ** (-0.5)
    pending = []

    def copy(src, dst, send_sem, recv_sem, to_d, to_t):
        return pltpu.make_async_remote_copy(
            src_ref=src, dst_ref=dst, send_sem=send_sem, recv_sem=recv_sem,
            device_id={"dp": to_d, "tensor": to_t}, device_id_type=MESH,
        )

    barrier = pltpu.get_barrier_semaphore()
    for k in range(1, seqs):
        pl.semaphore_signal(
            barrier, inc=1, device_id={"dp": lax.rem(d + k, seqs), "tensor": t},
            device_id_type=MESH,
        )
    for k in range(1, line):
        pl.semaphore_signal(
            barrier, inc=1, device_id={"dp": d, "tensor": lax.rem(t + k, line)},
            device_id_type=MESH,
        )
    pl.semaphore_signal(
        barrier, inc=1, device_id={"groups": 1 - g, "dp": d, "tensor": t}, device_id_type=MESH
    )
    pl.semaphore_wait(barrier, seqs + line - 1)

    others = [lax.rem(d + k, seqs) for k in range(1, seqs)]
    peers = [lax.rem(t + k, line) for k in range(1, line)]
    mine = pl.ds(pl.multiple_of(d * rows, rows), rows)
    right = jnp.minimum(t + 1, line - 1)
    left = jnp.maximum(t - 1, 0)

    def send_upstream(c):
        for o in others:
            off = pl.multiple_of(o * features + c * wide, wide)
            one = copy(
                upstream.at[:, pl.ds(off, wide)], up_all.at[c, mine],
                up_send.at[o, c], up_recv.at[d, c], o, t,
            )
            one.start()
            pending.append((None, one))

    def wait_upstream(c):
        for o in others:
            dst = up_all.at[c, pl.ds(pl.multiple_of(o * rows, rows), rows)]
            copy(dst, dst, up_send.at[o, c], up_recv.at[o, c], o, t).wait_recv()

    def block(j, p):
        return proj_all.at[pl.ds(pl.multiple_of(j * high + p * half, half), half)]

    def proj_send(j, source, where, toward, run=True, keep=True):
        sems = right_send if toward is right else left_send
        one = copy(source, block(j, g), sems.at[j], proj_recv.at[j], d, toward)
        if run:

            @pl.when(where)
            def _():
                one.start()

        if keep:
            pending.append((where, one))

    def proj_own():
        source = projection.at[pl.ds(pl.multiple_of(g * half, half), half)]
        proj_send(t, source, t < line - 1, right)
        proj_send(t, source, t > 0, left)

    def swap(j, p):
        return pltpu.make_async_remote_copy(
            src_ref=block(j, p), dst_ref=block(j, p), send_sem=swap_send.at[j],
            recv_sem=swap_recv.at[j], device_id={"groups": 1 - g, "dp": d, "tensor": t},
            device_id_type=MESH,
        )

    def proj_step(k, run=True):
        from_left, from_right = jnp.maximum(t - k, 0), jnp.minimum(t + k, line - 1)
        for j, here, toward, on in (
            (from_left, t >= k, right, t < line - 1),
            (from_right, t + k < line, left, t > 0),
        ):
            dst = block(j, g)
            across = swap(j, g)
            if not run:
                pending.append((here, across))
            else:

                @pl.when(here)
                def _(dst=dst, j=j, across=across):
                    copy(dst, dst, right_send.at[j], proj_recv.at[j], d, right).wait_recv()
                    across.start()

            if k < line - 1:
                proj_send(j, dst, jnp.logical_and(here, on), toward, run, not run)

    def wait_swaps():
        for j in peers:
            swap(j, 1 - g).wait_recv()

    early = max(1, chunks // 4)
    for c in range(early):
        send_upstream(c)
    proj_own()

    ends = []
    sofar = lengths[0, 0]
    for n in range(lengths.shape[1]):
        ends.append(sofar)
        if n + 1 < lengths.shape[1]:
            sofar = sofar + lengths[0, n + 1]
    down = lax.broadcasted_iota(jnp.int32, (total, 1), 0)
    across = lax.broadcasted_iota(jnp.int32, (1, total), 1)
    label_down = sum((down >= e).astype(jnp.int32) for e in ends)
    label_across = sum((across >= e).astype(jnp.int32) for e in ends)
    for q in range(line):
        span = slice(q * rows, (q + 1) * rows)
        scores = dot(query[span, :], keys[...], 1, 1) * scaling
        allowed = jnp.logical_and(label_down[span] == label_across, across <= down[span])
        scores = jnp.where(allowed, scores, -1e30)
        exponent = jnp.exp(scores - jnp.max(scores, axis=1, keepdims=True))
        probs = exponent / jnp.sum(exponent, axis=1, keepdims=True)
        probs_ref[span, :] = probs
        att_own[q] = dot(probs.astype(BF16), values[...], 1, 0).astype(BF16)
    att_all[t, mine] = att_own[t]
    for o in peers:
        one = copy(
            att_own.at[o], att_all.at[t, mine], att_send.at[o], att_recv.at[t], d, o
        )
        one.start()
        pending.append((None, one))
    for c in range(chunks):
        up_all[c, mine] = upstream[:, pl.ds(pl.multiple_of(d * features + c * wide, wide), wide)]
    proj_all[pl.ds(pl.multiple_of(t * high, high), high), :] = projection[...]
    for o in peers:
        dst = att_all.at[o, mine]
        copy(dst, dst, att_send.at[o], att_recv.at[o], d, o).wait_recv()
    for o in others:
        one = copy(
            att_all.at[:, mine], att_all.at[:, mine], spread_send.at[o], spread_recv.at[d], o, t
        )
        one.start()
        pending.append((None, one))
    for c in range(early, chunks):
        send_upstream(c)
    proj_step(1)
    for o in others:
        dst = att_all.at[:, pl.ds(pl.multiple_of(o * rows, rows), rows)]
        copy(dst, dst, spread_send.at[o], spread_recv.at[o], o, t).wait_recv()

    def sum_chunk(c, run=True):
        for k in range(line - 1, 0, -1):
            for way, head, go, first, toward in (
                (0, jnp.minimum(t + k, line - 1), t + k < line, t == 0, right),
                (1, jnp.maximum(t - k, 0), t >= k, t == line - 1, left),
            ):
                one = copy(
                    stage.at[way, head, c], landed.at[way, head, c],
                    sum_send.at[way, head, c], sum_recv.at[way, head, c], d, toward,
                )

                if not run:
                    pending.append((go, one))
                    continue

                @pl.when(go)
                def _(way=way, head=head, first=first, one=one):
                    if c == 0:
                        att_turned[head] = att_all[head].T
                    term = dot(att_turned[head], up_all[c], 1, 0)

                    @pl.when(first)
                    def _():
                        stage[way, head, c] = term.astype(BF16)

                    @pl.when(jnp.logical_not(first))
                    def _():
                        one.wait_recv()
                        stage[way, head, c] = (
                            term + landed[way, head, c].astype(F32)
                        ).astype(BF16)

                    one.start()


    def own_term(c):
        cols = slice(c * wide, (c + 1) * wide)
        if c == 0:
            att_turned[t] = att_all[t].T
        grad_projection[:, cols] = dot(att_turned[t], up_all[c], 1, 0)

    def own_chunk(c):
        cols = slice(c * wide, (c + 1) * wide)
        for way, there in ((0, t > 0), (1, t < line - 1)):
            dst = landed.at[way, t, c]

            @pl.when(there)
            def _(way=way, dst=dst):
                copy(
                    dst, dst, sum_send.at[way, t, c], sum_recv.at[way, t, c], d, right
                ).wait_recv()
                grad_projection[:, cols] += landed[way, t, c].astype(F32)

    def part_copy(o):
        return copy(part.at[o], part_in.at[d], part_send.at[o], part_recv.at[d], o, t)

    def out_term(c):
        piece = dot(up_all[c], proj_all[:, c * wide:(c + 1) * wide], 1, 1)
        if c == 0:
            out_acc[...] = piece
        else:
            out_acc[...] += piece

    def out_partials():
        for o in others + [d]:
            at = pl.ds(pl.multiple_of(o * rows, rows), rows)
            if o is d:
                part_in[d] = out_acc[at, :].astype(BF16)
                continue
            part[o] = out_acc[at, :].astype(BF16)
            part_copy(o).start()

    def og_copy(o):
        return copy(og_own.at[o], og_in.at[t], og_send.at[o], og_recv.at[t], d, o)

    def out_sum():
        for o in others:
            dst = part_in.at[o]
            copy(dst, dst, part_send.at[o], part_recv.at[o], o, t).wait_recv()
        whole = sum(part_in[n].astype(F32) for n in range(seqs)).astype(BF16)
        for q in range(line):
            og_own[q] = whole[:, q * HD:(q + 1) * HD]
        og_in[t] = og_own[t]
        for o in peers:
            og_copy(o).start()

    inner = jnp.logical_and(t > 0, t < line - 1)
    outer = jnp.logical_not(inner)
    wait_upstream(0)
    for k in range(2, line - 1):

        @pl.when(inner)
        def _(k=k):
            proj_step(k)

    sum_chunk(0)
    for k in range(2, line - 1):

        @pl.when(outer)
        def _(k=k):
            proj_step(k)

    @pl.when(outer)
    def _():
        for c in range(1, chunks):
            wait_upstream(c)
            sum_chunk(c)
            if c == 1:
                proj_step(line - 1)
        wait_swaps()
        for c in range(chunks):
            out_term(c)
        out_partials()
        for c in range(chunks):
            own_term(c)
        out_sum()

    @pl.when(inner)
    def _():
        proj_step(line - 1)
        wait_swaps()
        for c in range(chunks):
            if c > 0:
                wait_upstream(c)
            out_term(c)
        out_partials()
        for c in range(1, chunks):
            sum_chunk(c)
            if c == 1:
                out_sum()
        for c in range(chunks):
            own_term(c)

    for o in peers:
        dst = og_in.at[o]
        copy(dst, dst, og_send.at[o], og_recv.at[o], d, o).wait_recv()
    grads = [og_in[q] for q in range(line)]
    gv = 0.0
    gk = 0.0
    for q in range(line):
        span = slice(q * rows, (q + 1) * rows)
        probs = probs_ref[span, :]
        gv = gv + dot(probs.astype(BF16), grads[q], 0, 0)
        grad_probs = dot(grads[q], values[...], 1, 1)
        delta = jnp.sum(probs * grad_probs, axis=1, keepdims=True)
        grad_scores = (probs * (grad_probs - delta) * scaling).astype(BF16)
        grad_query[span, :] = dot(grad_scores, keys[...], 1, 0).astype(BF16)
        gk = gk + dot(grad_scores, query[span, :], 0, 0)
    grad_values[...] = gv.astype(BF16)
    grad_keys[...] = gk.astype(BF16)
    for c in range(chunks):
        own_chunk(c)

    for o in others:
        pending.append((None, part_copy(o)))
    for o in peers:
        pending.append((None, og_copy(o)))
    for k in range(1, line):
        proj_step(k, False)
    for c in range(chunks):
        sum_chunk(c, False)
    for where, one in pending:
        if where is None:
            one.wait_send()
        else:

            @pl.when(where)
            def _(one=one):
                one.wait_send()


def hand_on(pieces, *refs):
    count = (len(refs) - 2) // 3
    ins, outs, held = refs[:count], refs[count:2 * count], refs[2 * count:3 * count]
    in_sems, out_sems = refs[3 * count:]
    steps = []
    for n, (i, o, h) in enumerate(zip(ins, outs, held)):
        size = i.shape[0] // pieces
        for p in range(pieces):
            at = pl.ds(p * size, size)
            steps.append((
                pltpu.make_async_copy(i.at[at], h.at[at], in_sems.at[n, p]),
                pltpu.make_async_copy(h.at[at], o.at[at], out_sems.at[n, p]),
            ))
    for take, _ in steps:
        take.start()
    for take, give in steps:
        take.wait()
        give.start()
    for _, give in steps:
        give.wait()


def handed_on(arrays, pieces=2):
    held = pl.BlockSpec(memory_space=pl.ANY)
    return pl.pallas_call(
        functools.partial(hand_on, pieces),
        out_shape=tuple(jax.ShapeDtypeStruct(a.shape, a.dtype) for a in arrays),
        in_specs=[held] * len(arrays),
        out_specs=(held,) * len(arrays),
        scratch_shapes=[pltpu.VMEM(a.shape, a.dtype) for a in arrays]
        + [pltpu.SemaphoreType.DMA((len(arrays), pieces))] * 2,
    )(*arrays)


def fused_shards(seqs, line, query, keys, values, upstream, projection, lengths):
    total, width = query.shape
    rows = upstream.shape[0]
    high, features = projection.shape
    chunks = CHUNKS
    wide = features // chunks
    dma = pltpu.SemaphoreType.DMA
    vmem = pltpu.VMEM
    whole = pl.BlockSpec(memory_space=pltpu.VMEM)
    grads = pl.pallas_call(
        functools.partial(kernel, seqs, line, chunks),
        out_shape=(
            jax.ShapeDtypeStruct(query.shape, BF16),
            jax.ShapeDtypeStruct(query.shape, BF16),
            jax.ShapeDtypeStruct(query.shape, BF16),
            jax.ShapeDtypeStruct(projection.shape, F32),
        ),
        in_specs=[whole] * 5 + [pl.BlockSpec(memory_space=pltpu.SMEM)],
        out_specs=(whole,) * 4,
        scratch_shapes=[
            vmem((total, total), F32),
            vmem((line, rows, width), BF16),
            vmem((line, seqs * rows, width), BF16),
            vmem((line, width, seqs * rows), BF16),
            vmem((seqs * rows, line * high), F32),
            vmem((chunks, seqs * rows, wide), BF16),
            vmem((line * high, features), BF16),
            vmem((seqs, rows, line * high), BF16),
            vmem((seqs, rows, line * high), BF16),
            vmem((line, rows, width), BF16),
            vmem((line, rows, width), BF16),
            vmem((2, line, chunks, high, wide), BF16),
            vmem((2, line, chunks, high, wide), BF16),
            dma((seqs, chunks)), dma((seqs, chunks)),
            dma((line,)), dma((line,)), dma((line,)), dma((line,)), dma((line,)),
            dma((line,)), dma((line,)),
            dma((seqs,)), dma((seqs,)),
            dma((seqs,)), dma((seqs,)),
            dma((line,)), dma((line,)),
            dma((2, line, chunks)), dma((2, line, chunks)),
        ],
        compiler_params=pltpu.CompilerParams(collective_id=0, has_side_effects=True),
    )(query, keys, values, upstream, projection, lengths)
    return handed_on(grads)


def solution(mesh):
    seqs, line = mesh.shape["dp"], mesh.shape["tensor"]

    def shards(query, keys, values, upstream, projection, lengths):
        fits = (
            query.shape[1] == HD
            and projection.shape[0] == HD
            and 1 < seqs
            and 1 < line
            and max(seqs, line) <= MOST_STEPS
            and projection.shape[1] % (CHUNKS * LANES) == 0
            and upstream.shape[0] % 32 == 0
            and mesh.shape["groups"] == 2
            and 3 <= line
            and upstream.shape[0] * line == query.shape[0]
        )
        if fits:
            return fused_shards(seqs, line, query, keys, values, upstream, projection, lengths)
        return plain_shards(query, keys, values, upstream, projection, lengths)

    in_specs = (
        P(("groups", "dp"), "tensor"),
        P(("groups", "dp"), "tensor"),
        P(("groups", "dp"), "tensor"),
        P(("groups", "dp", "tensor"), None),
        P("tensor", "dp"),
        P(("groups", "dp"), None),
    )
    out_specs = (
        P(("groups", "dp"), "tensor"),
        P(("groups", "dp"), "tensor"),
        P(("groups", "dp"), "tensor"),
        P(("groups", "tensor"), "dp"),
    )
    return jax.shard_map(shards, mesh=mesh, in_specs=in_specs, out_specs=out_specs, check_vma=False)
```
